16 devices in a mesh: dp: 1, sp: 16 (over x, y, z, core).
Axes of the slice: x: 2, y: 2, z: 2, core: 2. Of those that a mesh axis runs over, the one named last changes fastest.
Arguments:
- q: bfloat16 [32, 64, 112], P('dp')
- k: bfloat16 [32, 4096, 64, 112], P('dp', 'sp')
- v: bfloat16 [32, 4096, 64, 112], P('dp', 'sp')
Outputs:
- q: bfloat16 [32, 64, 112], P('dp')
All inputs are finite; a program needn't handle non-finite values.
Results may differ from the reference program's by a relative error of at most 0.012.
Values are sent between devices in bfloat16 or wider.
A program may use at most 2 GiB of HBM per device.

```python
import jax
import jax.numpy as jnp

BATCH = 32
CACHE = 4096
HEADS = 64
KV_HEADS = 64
HEAD = 112


def setup_inputs(seed: int = 0, part: int = 0) -> dict:
    kq, kk, kv = (jax.random.fold_in(k, part) for k in jax.random.split(jax.random.key(seed), 3))
    return {
        "q": (3 * jax.random.normal(kq, (BATCH, HEADS, HEAD), jnp.float32)).astype(jnp.bfloat16),
        "k": jax.random.normal(kk, (BATCH, CACHE, KV_HEADS, HEAD), jnp.float32).astype(jnp.bfloat16),
        "v": jax.random.normal(kv, (BATCH, CACHE, KV_HEADS, HEAD), jnp.float32).astype(jnp.bfloat16),
    }


def einsum(form, a, b):
    return jnp.einsum(form, a.astype(jnp.float32), b.astype(jnp.float32))


def reference(q, k, v):
    grouped = q.reshape(BATCH, KV_HEADS, -1, HEAD)
    scores = einsum("bgsd,bugd->bgsu", grouped, k) * HEAD**-0.5
    weights = jax.nn.softmax(scores, -1).astype(jnp.bfloat16)
    return einsum("bgsu,bugd->bgsd", weights, v).astype(jnp.bfloat16).reshape(BATCH, HEADS, HEAD)
```

```python
import functools

import jax
import jax.numpy as jnp
from jax import lax
from jax.experimental import pallas as pl
from jax.experimental.pallas import tpu as pltpu
from jax.sharding import PartitionSpec as P

HIGH, TOTAL, ROW = 112, 120, 128
GROUP = 16
SLOTS = 3
SENDS = 4


def masked(x):
    shape = (x.shape[0], *x.shape)
    keep = lax.broadcasted_iota(jnp.int32, shape, 0) == lax.broadcasted_iota(jnp.int32, shape, 1)
    return jnp.where(keep, x[None], jnp.zeros((), x.dtype))


def weights_of(q, k):
    each = lax.dot_general(masked(q), k, (((2,), (1,)), ((0,), (0,))), preferred_element_type=jnp.float32)
    scores = jnp.sum(each, 0) * q.shape[1] ** -0.5
    high = jnp.max(scores, -1, keepdims=True)
    weights = jnp.exp(scores - high)
    return weights.astype(q.dtype), high, jnp.sum(weights, -1, keepdims=True)


def seen_of(weights, v):
    each = lax.dot_general(masked(weights), v, (((2,), (2,)), ((0,), (0,))), preferred_element_type=jnp.float32)
    return jnp.sum(each, 0)


def kernel(n, q_hbm, k_ref, v_ref, out_ref, q_ref, keys, values, part, got, held, q_sem, k_sem, v_sem, part_sem, got_sem, send_sem, out_sem):
    me = lax.axis_index("sp")
    batch, heads, _ = q_ref.shape
    own, groups = batch // n, heads // GROUP
    sent = batch - own
    first = lax.rem((me + 1) * own, batch)

    def rows(g):
        return pl.ds(g * GROUP, GROUP)

    def sequence(j):
        return lax.rem(first + j, batch)

    def fetch_k(j):
        slot = lax.rem(j, SLOTS)
        return pltpu.make_async_copy(k_ref.at[sequence(j)], keys.at[slot], k_sem.at[slot])

    def fetch_v(j, g):
        slot = lax.rem(j, SLOTS)
        return pltpu.make_async_copy(v_ref.at[sequence(j), rows(g)], values.at[slot, rows(g)], v_sem.at[slot, g])

    def fetch(j):
        fetch_k(j).start()
        for g in range(groups):
            fetch_v(j, g).start()

    def other(step):
        return sum(bit * lax.rem(lax.div(me, bit) + lax.div(step, bit), 2) for bit in (1, 2, 4, 8))

    def to(place):
        return dict(device_id={"sp": place}, device_id_type=pl.DeviceIdType.MESH)

    query = pltpu.make_async_copy(q_hbm, q_ref, q_sem)
    query.start()
    for j in range(SLOTS):
        fetch(j)

    barrier = pltpu.get_barrier_semaphore()

    @pl.loop(1, n)
    def _(step):
        pl.semaphore_signal(barrier, inc=1, **to(other(step)))

    pl.semaphore_wait(barrier, n - 1)
    query.wait()

    lane = lax.broadcasted_iota(jnp.int32, (heads, ROW), 1)
    for u in range(own):
        got[u, me] = jnp.where((lane >= HIGH) & (lane < TOTAL), jnp.finfo(jnp.float32).min, 0.0)

    def send_part(j):
        slot, b = lax.rem(j, SENDS), sequence(j)
        u = lax.rem(b, own)
        return pltpu.make_async_remote_copy(part.at[slot], got.at[u, me], part_sem.at[slot], got_sem.at[u, me], **to(lax.div(b, own)))

    @pl.loop(0, sent)
    def _(j):
        slot, b, turn = lax.rem(j, SLOTS), sequence(j), lax.rem(j, SENDS)
        fetch_k(j).wait()
        for g in range(groups):
            fetch_v(j, g).wait()

        @pl.when(j >= SENDS)
        def _():
            send_part(j - SENDS).wait_send()

        for g in range(groups):
            at = rows(g)
            weights, high, total = weights_of(q_ref[b, at], keys[slot, at])
            part[turn, at, :HIGH] = seen_of(weights, values[slot, at])
            part[turn, at, HIGH:TOTAL] = jnp.broadcast_to(high, (GROUP, TOTAL - HIGH))
            part[turn, at, TOTAL:] = jnp.broadcast_to(total, (GROUP, ROW - TOTAL))
        send_part(j).start()

        @pl.when(j + SLOTS < batch)
        def _():
            fetch(j + SLOTS)

    def send_out(u, g, step):
        at = out_ref.at[me * own + u, rows(g)]
        return pltpu.make_async_remote_copy(at, at, send_sem.at[u, g, step], out_sem.at[u, g, me], **to(other(step)))

    @pl.loop(0, own)
    def _(u):
        j = sent + u
        slot, b = lax.rem(j, SLOTS), sequence(j)

        @pl.loop(1, n)
        def _(step):
            at = got.at[u, other(step)]
            pltpu.make_async_copy(at, at, got_sem.at[u, other(step)]).wait()

        for g in range(groups):
            parts = got[u, :, rows(g)]
            high = jnp.max(parts[:, :, HIGH:HIGH + 1], 0)
            put = jnp.sum(parts * jnp.exp(parts[:, :, HIGH:HIGH + 1] - high[None]), 0)
            held[0, rows(g)] = put
            held[1, rows(g)] = jnp.broadcast_to(high, (GROUP, ROW))

        fetch_k(j).wait()
        mine = [weights_of(q_ref[b, rows(g)], keys[slot, rows(g)]) for g in range(groups)]
        for g in range(groups):
            weights, high, total = mine[g]
            fetch_v(j, g).wait()
            seen = seen_of(weights, values[slot, rows(g)])
            theirs = held[1, rows(g), :1]
            both = jnp.maximum(theirs, high)
            old, new = jnp.exp(theirs - both), jnp.exp(high - both)
            put = held[0, rows(g)] * old
            out_ref[b, rows(g)] = ((put[:, :HIGH] + seen * new) / (put[:, TOTAL:TOTAL + 1] + total * new)).astype(out_ref.dtype)

            @pl.loop(1, n)
            def _(step):
                send_out(u, g, n - step).start()

    @pl.loop(sent - SENDS, sent)
    def _(j):
        send_part(j).wait_send()

    @pl.loop(0, own)
    def _(u):
        @pl.loop(0, groups)
        def _(g):
            @pl.loop(1, n)
            def _(step):
                send_out(u, g, step).wait_send()
                place = other(step)
                at = out_ref.at[place * own + u, rows(g)]
                pltpu.make_async_copy(at, at, out_sem.at[u, g, place]).wait()


def solution(mesh):
    n = mesh.shape["sp"]

    def step(q, k, v):
        batch, keys, heads, head = k.shape
        own, groups = batch // n, heads // GROUP
        return pl.pallas_call(
            functools.partial(kernel, n),
            out_shape=jax.ShapeDtypeStruct(q.shape, q.dtype),
            in_specs=[pl.BlockSpec(memory_space=pl.ANY)] * 3,
            out_specs=pl.BlockSpec(memory_space=pltpu.VMEM),
            scratch_shapes=[
                pltpu.VMEM(q.shape, q.dtype),
                pltpu.VMEM((SLOTS, heads, head, keys), k.dtype),
                pltpu.VMEM((SLOTS, heads, head, keys), v.dtype),
                pltpu.VMEM((SENDS, heads, ROW), jnp.float32),
                pltpu.VMEM((own, n, heads, ROW), jnp.float32),
                pltpu.VMEM((2, heads, ROW), jnp.float32),
                pltpu.SemaphoreType.DMA,
                pltpu.SemaphoreType.DMA((SLOTS,)),
                pltpu.SemaphoreType.DMA((SLOTS, groups)),
                pltpu.SemaphoreType.DMA((SENDS,)),
                pltpu.SemaphoreType.DMA((own, n)),
                pltpu.SemaphoreType.DMA((own, groups, n)),
                pltpu.SemaphoreType.DMA((own, groups, n)),
            ],
            compiler_params=pltpu.CompilerParams(collective_id=0, has_side_effects=True, vmem_limit_bytes=60 * 2**20),
        )(q, jnp.transpose(k, (0, 2, 3, 1)), jnp.transpose(v, (0, 2, 3, 1)))

    return jax.shard_map(
        step,
        mesh=mesh,
        in_specs=(P("dp", None, None), P("dp", "sp", None, None), P("dp", "sp", None, None)),
        out_specs=P("dp", None, None),
        check_vma=False,
    )
```

```python
import functools

import jax
import jax.numpy as jnp
from jax import lax
from jax.experimental import pallas as pl
from jax.experimental.pallas import tpu as pltpu
from jax.sharding import PartitionSpec as P

HIGH, TOTAL, ROW = 112, 120, 128
GROUP = 16
STEP = 32
SLOTS = 6
SENDS = 4


def alone(x, h):
    return jnp.where(lax.broadcasted_iota(jnp.int32, (x.shape[0], 1), 0) == h, x, jnp.zeros((), x.dtype))


def over_heads(x, other, contract):
    each = [lax.dot_general(alone(x, h), other(h), ((contract[:1], contract[1:]), ((), ())), preferred_element_type=jnp.float32) for h in range(GROUP)]
    even = lax.rem(lax.broadcasted_iota(jnp.int32, (GROUP, 1), 0), 2) == 0
    return jnp.where(even, sum(each[2::2], each[0]), sum(each[3::2], each[1]))


def weights_of(q, k):
    scores = over_heads(q, k, (1, 0)) * q.shape[1] ** -0.5
    high = jnp.max(scores, -1, keepdims=True)
    weights = jnp.exp(scores - high)
    return weights.astype(q.dtype), high, jnp.sum(weights, -1, keepdims=True)


def kernel(n, q_hbm, k_ref, v_ref, out_ref, q_ref, keys, values, part, got, held, q_sem, k_sem, v_sem, part_sem, got_sem, send_sem, out_sem):
    me = lax.axis_index("sp")
    batch, heads, _ = q_ref.shape
    own, halves, groups = batch // n, heads // STEP, STEP // GROUP
    rounds = own * halves
    steps = rounds * n

    def other(flip):
        return sum(bit * lax.rem(lax.div(me, bit) + lax.div(flip, bit), 2) for bit in (1, 2, 4, 8))

    def to(place):
        return dict(device_id={"sp": place}, device_id_type=pl.DeviceIdType.MESH)

    def owner(j):
        return other(n - 1 - lax.rem(j, n))

    def rows_of(place, r):
        return place * own + lax.div(r, halves), pl.multiple_of(lax.rem(r, halves) * STEP, STEP)

    def group(start, g):
        return pl.ds(pl.multiple_of(start + g * GROUP, GROUP), GROUP)

    def fetch_k(j):
        b, start = rows_of(owner(j), lax.div(j, n))
        slot = lax.rem(j, SLOTS)
        return pltpu.make_async_copy(k_ref.at[b, pl.ds(start, STEP)], keys.at[slot], k_sem.at[slot])

    def fetch_v(j, g):
        b, start = rows_of(owner(j), lax.div(j, n))
        slot = lax.rem(j, SLOTS)
        return pltpu.make_async_copy(v_ref.at[b, group(start, g)], values.at[slot, group(0, g)], v_sem.at[slot, g])

    def fetch(j):
        fetch_k(j).start()

        @pl.loop(0, groups)
        def _(g):
            fetch_v(j, g).start()

    def wait(ref, sem):
        pltpu.make_async_copy(ref, ref, sem).wait()

    query = pltpu.make_async_copy(q_hbm, q_ref, q_sem)
    query.start()

    @pl.loop(0, SLOTS)
    def _(j):
        fetch(j)

    barrier = pltpu.get_barrier_semaphore()

    @pl.loop(1, n)
    def _(flip):
        pl.semaphore_signal(barrier, inc=1, **to(other(flip)))

    pl.semaphore_wait(barrier, n - 1)
    query.wait()

    lane = lax.broadcasted_iota(jnp.int32, (STEP, ROW), 1)
    for r in range(rounds):
        got[r, me] = jnp.where((lane >= HIGH) & (lane < TOTAL), jnp.finfo(jnp.float32).min, 0.0)

    def next_fetch(j):
        @pl.when(j + SLOTS < steps)
        def _():
            fetch(j + SLOTS)

    @pl.loop(0, rounds)
    def _(r):
        @pl.loop(0, n - 1)
        def _(i):
            j = r * n + i
            place = owner(j)
            b, start = rows_of(place, r)
            slot, turn = lax.rem(j, SLOTS), lax.rem(r * (n - 1) + i, SENDS)
            fetch_k(j).wait()
            for g in range(groups):
                fetch_v(j, g).wait()

            @pl.when(r * (n - 1) + i >= SENDS)
            def _():
                wait(part.at[turn], part_sem.at[turn])

            mine = [weights_of(q_ref[b, group(start, g)], lambda h: keys[slot, g * GROUP + h]) for g in range(groups)]
            for g in range(groups):
                at = group(0, g)
                weights, high, total = mine[g]
                part[turn, at, :HIGH] = over_heads(weights, lambda h: values[slot, g * GROUP + h], (1, 1))
                part[turn, at, HIGH:TOTAL] = jnp.broadcast_to(high, (GROUP, TOTAL - HIGH))
                part[turn, at, TOTAL:] = jnp.broadcast_to(total, (GROUP, ROW - TOTAL))
            pltpu.make_async_remote_copy(part.at[turn], got.at[r, me], part_sem.at[turn], got_sem.at[r], **to(place)).start()
            next_fetch(j)

        j = r * n + n - 1
        b, start = rows_of(me, r)
        slot = lax.rem(j, SLOTS)
        fetch_k(j).wait()
        mine = [weights_of(q_ref[b, group(start, g)], lambda h: keys[slot, g * GROUP + h]) for g in range(groups)]

        wait(got.at[r, pl.ds(0, n - 1)], got_sem.at[r])
        for g in range(groups):
            parts = got[r, :, group(0, g)]
            high = jnp.max(parts[:, :, HIGH:HIGH + 1], 0)
            held[0, group(0, g)] = jnp.sum(parts * jnp.exp(parts[:, :, HIGH:HIGH + 1] - high[None]), 0)
            held[1, group(0, g)] = jnp.broadcast_to(high, (GROUP, ROW))

        for g in range(groups):
            weights, high, total = mine[g]
            fetch_v(j, g).wait()
            seen = over_heads(weights, lambda h: values[slot, g * GROUP + h], (1, 1))
            theirs = held[1, group(0, g), :1]
            both = jnp.maximum(theirs, high)
            old, new = jnp.exp(theirs - both), jnp.exp(high - both)
            put = held[0, group(0, g)] * old
            at = out_ref.at[b, group(start, g)]
            at[...] = ((put[:, :HIGH] + seen * new) / (put[:, TOTAL:TOTAL + 1] + total * new)).astype(out_ref.dtype)
            for flip in range(n - 1, 0, -1):
                pltpu.make_async_remote_copy(at, at, send_sem, out_sem, **to(other(flip))).start()
        next_fetch(j)

    for turn in range(SENDS):
        wait(part.at[turn], part_sem.at[turn])
    wait(out_ref.at[pl.ds(0, batch - own)], send_sem)
    wait(out_ref.at[pl.ds(0, batch - own)], out_sem)


def solution(mesh):
    n = mesh.shape["sp"]

    def step(q, k, v):
        batch, keys, heads, head = k.shape
        rounds, groups = batch * heads // STEP // n, STEP // GROUP
        return pl.pallas_call(
            functools.partial(kernel, n),
            out_shape=jax.ShapeDtypeStruct(q.shape, q.dtype),
            in_specs=[pl.BlockSpec(memory_space=pl.ANY)] * 3,
            out_specs=pl.BlockSpec(memory_space=pltpu.VMEM),
            scratch_shapes=[
                pltpu.VMEM(q.shape, q.dtype),
                pltpu.VMEM((SLOTS, STEP, head, keys), k.dtype),
                pltpu.VMEM((SLOTS, STEP, head, keys), v.dtype),
                pltpu.VMEM((SENDS, STEP, ROW), jnp.float32),
                pltpu.VMEM((rounds, n, STEP, ROW), jnp.float32),
                pltpu.VMEM((2, STEP, ROW), jnp.float32),
                pltpu.SemaphoreType.DMA,
                pltpu.SemaphoreType.DMA((SLOTS,)),
                pltpu.SemaphoreType.DMA((SLOTS, groups)),
                pltpu.SemaphoreType.DMA((SENDS,)),
                pltpu.SemaphoreType.DMA((rounds,)),
                pltpu.SemaphoreType.DMA,
                pltpu.SemaphoreType.DMA,
            ],
            compiler_params=pltpu.CompilerParams(collective_id=0, has_side_effects=True, vmem_limit_bytes=48 * 2**20),
        )(pltpu.with_memory_space_constraint(q, pltpu.HBM), jnp.transpose(k, (0, 2, 3, 1)), jnp.transpose(v, (0, 2, 3, 1)))

    return jax.shard_map(
        step,
        mesh=mesh,
        in_specs=(P("dp", None, None), P("dp", "sp", None, None), P("dp", "sp", None, None)),
        out_specs=P("dp", None, None),
        check_vma=False,
    )
```

```python
import functools

import jax
import jax.numpy as jnp
from jax import lax
from jax.experimental import pallas as pl
from jax.experimental.pallas import tpu as pltpu
from jax.sharding import PartitionSpec as P

HIGH, TOTAL, ROW = 112, 120, 128
GROUP = 16
STEP = 32
SLOTS = 6
SENDS = 4


def alone(x, h):
    return jnp.where(lax.broadcasted_iota(jnp.int32, (x.shape[0], 1), 0) == h, x, jnp.zeros((), x.dtype))


def over_heads(x, other, contract):
    each = [lax.dot_general(alone(x, h), other(h), ((contract[:1], contract[1:]), ((), ())), preferred_element_type=jnp.float32) for h in range(GROUP)]
    even = lax.rem(lax.broadcasted_iota(jnp.int32, (GROUP, 1), 0), 2) == 0
    return jnp.where(even, sum(each[2::2], each[0]), sum(each[3::2], each[1]))


def weights_of(q, k):
    scores = over_heads(q, k, (1, 0)) * q.shape[1] ** -0.5
    high = jnp.max(scores, -1, keepdims=True)
    weights = jnp.exp(scores - high)
    return weights.astype(q.dtype), high, jnp.sum(weights, -1, keepdims=True)


def kernel(n, q_hbm, k_ref, v_ref, out_ref, q_ref, keys, values, part, got, kept, kept_high, kept_total, q_sem, k_sem, v_sem, part_sem, got_sem, send_sem, out_sem):
    me = lax.axis_index("sp")
    batch, heads, _ = q_ref.shape
    rounds, halves, groups = batch // n, heads // STEP, STEP // GROUP
    turns = n * halves
    steps = rounds * turns

    def other(flip):
        return sum(bit * lax.rem(lax.div(me, bit) + lax.div(flip, bit), 2) for bit in (1, 2, 4, 8))

    def to(place):
        return dict(device_id={"sp": place}, device_id_type=pl.DeviceIdType.MESH)

    def owner(j):
        return other(n - 1 - lax.div(lax.rem(j, turns), halves))

    def rows_of(j):
        return owner(j) * rounds + lax.div(j, turns), pl.multiple_of(lax.rem(j, halves) * STEP, STEP)

    def group(start, g):
        return pl.ds(pl.multiple_of(start + g * GROUP, GROUP), GROUP)

    def fetch_k(j):
        b, start = rows_of(j)
        slot = lax.rem(j, SLOTS)
        return pltpu.make_async_copy(k_ref.at[b, pl.ds(start, STEP)], keys.at[slot], k_sem.at[slot])

    def value_copy(j, g):
        b, start = rows_of(j)
        slot = lax.rem(j, SLOTS)
        return pltpu.make_async_copy(v_ref.at[b, group(start, g)], values.at[slot, group(0, g)], v_sem.at[slot, g])

    def fetch_v(j):
        @pl.loop(0, groups)
        def _(g):
            value_copy(j, g).start()

    def wait(ref, sem):
        pltpu.make_async_copy(ref, ref, sem).wait()

    query = pltpu.make_async_copy(q_hbm, q_ref, q_sem)
    query.start()

    fetch_k(0).start()

    @pl.loop(1, SLOTS)
    def _(j):
        fetch_k(j).start()
        fetch_v(j - 1)

    fetch_v(SLOTS - 1)

    barrier = pltpu.get_barrier_semaphore()

    @pl.loop(1, n)
    def _(flip):
        pl.semaphore_signal(barrier, inc=1, **to(other(flip)))

    pl.semaphore_wait(barrier, n - 1)
    query.wait()

    def weigh(j):
        b, start = rows_of(j)
        slot, turn = lax.rem(j, SLOTS), lax.rem(j, 2)
        for g in range(groups):
            weights, high, total = weights_of(q_ref[b, group(start, g)], lambda h: keys[slot, g * GROUP + h])
            kept[turn, group(0, g)] = weights
            kept_high[turn, group(0, g)] = jnp.broadcast_to(high, (GROUP, ROW))
            kept_total[turn, group(0, g)] = jnp.broadcast_to(total, (GROUP, ROW))

    def seen_of(j, g):
        slot, turn = lax.rem(j, SLOTS), lax.rem(j, 2)
        return over_heads(kept[turn, group(0, g)], lambda h: values[slot, g * GROUP + h], (1, 1))

    def next_fetch(j):
        @pl.when(j + 1 + SLOTS < steps)
        def _():
            fetch_k(j + 1 + SLOTS).start()

        @pl.when(j + SLOTS < steps)
        def _():
            fetch_v(j + SLOTS)

    def send_out(rows, flip):
        pltpu.make_async_remote_copy(rows, rows, send_sem, out_sem, **to(other(flip))).start()

    hops = {flip: (flip // 2).bit_count() for flip in range(1, n)}
    far = [flip for flip in sorted(hops, key=lambda flip: (-hops[flip], -(flip // 2), flip % 2)) if hops[flip] > 1]
    close = [flip for flip in range(n - 1, 0, -1) if hops[flip] < 2]

    fetch_k(0).wait()
    weigh(0)
    fetch_k(SLOTS).start()

    @pl.loop(0, rounds)
    def _(r):
        @pl.loop(0, turns - halves)
        def _(i):
            j, sent = r * turns + i, r * (turns - halves) + i
            place, half = owner(j), lax.rem(i, halves)
            turn, to_send = lax.rem(j, 2), lax.rem(sent, SENDS)
            fetch_k(j + 1).wait()
            for g in range(groups):
                value_copy(j, g).wait()

            @pl.when(sent >= SENDS)
            def _():
                wait(part.at[to_send], part_sem.at[to_send])

            weigh(j + 1)
            for g in range(groups):
                at = group(0, g)
                part[to_send, at, :HIGH] = seen_of(j, g)
                part[to_send, at, HIGH:TOTAL] = kept_high[turn, at, HIGH:TOTAL]
                part[to_send, at, TOTAL:] = kept_total[turn, at, TOTAL:]
            near = lax.div(i, halves * (n - 2))
            pltpu.make_async_remote_copy(part.at[to_send], got.at[r, half, me], part_sem.at[to_send], got_sem.at[r, half, near], **to(place)).start()
            next_fetch(j)

        for half in range(halves):
            j = (r + 1) * turns - halves + half
            b, start = rows_of(j)
            turn, last = lax.rem(j, 2), half == halves - 1
            seen = []
            if last:
                for g in range(groups - 1):
                    value_copy(j, g).wait()
                    seen.append(seen_of(j, g))
            else:
                fetch_k(j + 1).wait()
            for g in range(len(seen), groups):
                value_copy(j, g).wait()
            wait(got.at[r, half, pl.ds(0, n - 2)], got_sem.at[r, half, 0])
            wait(got.at[r, half, other(1)], got_sem.at[r, half, 1])
            if not last:
                weigh(j + 1)
            seen += [seen_of(j, g) for g in range(len(seen), groups)]
            for g in range(groups):
                parts = [got[r, half, other(flip), group(0, g)] for flip in range(1, n)]
                high = kept_high[turn, group(0, g), :1]
                top = functools.reduce(jnp.maximum, [x[:, HIGH:HIGH + 1] for x in parts], high)
                new = jnp.exp(high - top)
                rest = sum(x * jnp.exp(x[:, HIGH:HIGH + 1] - top) for x in parts)
                total = rest[:, TOTAL:TOTAL + 1] + kept_total[turn, group(0, g), :1] * new
                at = out_ref.at[b, group(start, g)]
                at[...] = (rest[:, :HIGH] / total + seen[g] * (new / total)).astype(out_ref.dtype)
            for flip in far:
                send_out(out_ref.at[b, pl.ds(start, STEP)], flip)
            if last:
                for flip in close:
                    send_out(out_ref.at[b], flip)

                @pl.when(j + 1 < steps)
                def _():
                    fetch_k(j + 1).wait()
                    weigh(j + 1)
            next_fetch(j)

    for turn in range(SENDS):
        wait(part.at[turn], part_sem.at[turn])
    wait(out_ref.at[pl.ds(0, batch - rounds)], send_sem)
    wait(out_ref.at[pl.ds(0, batch - rounds)], out_sem)


def solution(mesh):
    n = mesh.shape["sp"]

    def step(q, k, v):
        batch, keys, heads, head = k.shape
        rounds, halves, groups = batch // n, heads // STEP, STEP // GROUP
        return pl.pallas_call(
            functools.partial(kernel, n),
            out_shape=jax.ShapeDtypeStruct(q.shape, q.dtype),
            in_specs=[pl.BlockSpec(memory_space=pl.ANY)] * 3,
            out_specs=pl.BlockSpec(memory_space=pltpu.VMEM),
            scratch_shapes=[
                pltpu.VMEM(q.shape, q.dtype),
                pltpu.VMEM((SLOTS, STEP, head, keys), k.dtype),
                pltpu.VMEM((SLOTS, STEP, head, keys), v.dtype),
                pltpu.VMEM((SENDS, STEP, ROW), jnp.float32),
                pltpu.VMEM((rounds, halves, n, STEP, ROW), jnp.float32),
                pltpu.VMEM((2, STEP, keys), q.dtype),
                pltpu.VMEM((2, STEP, ROW), jnp.float32),
                pltpu.VMEM((2, STEP, ROW), jnp.float32),
                pltpu.SemaphoreType.DMA,
                pltpu.SemaphoreType.DMA((SLOTS,)),
                pltpu.SemaphoreType.DMA((SLOTS, groups)),
                pltpu.SemaphoreType.DMA((SENDS,)),
                pltpu.SemaphoreType.DMA((rounds, halves, 2)),
                pltpu.SemaphoreType.DMA,
                pltpu.SemaphoreType.DMA,
            ],
            compiler_params=pltpu.CompilerParams(collective_id=0, has_side_effects=True, vmem_limit_bytes=48 * 2**20),
        )(pltpu.with_memory_space_constraint(q, pltpu.HBM), jnp.transpose(k, (0, 2, 3, 1)), jnp.transpose(v, (0, 2, 3, 1)))

    return jax.shard_map(
        step,
        mesh=mesh,
        in_specs=(P("dp", None, None), P("dp", "sp", None, None), P("dp", "sp", None, None)),
        out_specs=P("dp", None, None),
        check_vma=False,
    )
```

```python
import functools

import jax
import jax.numpy as jnp
from jax import lax
from jax.experimental import pallas as pl
from jax.experimental.pallas import tpu as pltpu
from jax.sharding import PartitionSpec as P

HIGH, TOTAL, ROW = 112, 120, 128
GROUP = 16
STEP = 32
SLOTS = 8
SENDS = 4
AHEAD = 2


def alone(x, h):
    return jnp.where(lax.broadcasted_iota(jnp.int32, (x.shape[0], 1), 0) == h, x, jnp.zeros((), x.dtype))


def over_heads(x, other, contract):
    each = [lax.dot_general(alone(x, h), other(h), ((contract[:1], contract[1:]), ((), ())), preferred_element_type=jnp.float32) for h in range(GROUP)]
    even = lax.rem(lax.broadcasted_iota(jnp.int32, (GROUP, 1), 0), 2) == 0
    return jnp.where(even, sum(each[2::2], each[0]), sum(each[3::2], each[1]))


def weights_of(q, k):
    scores = over_heads(q, k, (1, 0)) * q.shape[1] ** -0.5
    high = jnp.max(scores, -1, keepdims=True)
    weights = jnp.exp(scores - high)
    return weights.astype(q.dtype), high, jnp.sum(weights, -1, keepdims=True)


def kernel(n, q_hbm, k_ref, v_ref, out_ref, q_ref, keys, values, part, got, kept, kept_high, kept_total, q_sem, k_sem, v_sem, part_sem, got_sem, send_sem, out_sem):
    me = lax.axis_index("sp")
    batch, heads, _ = q_ref.shape
    rounds, halves, groups = batch // n, heads // STEP, STEP // GROUP
    turns = n * halves
    steps = rounds * turns

    def other(flip):
        return sum(bit * lax.rem(lax.div(me, bit) + lax.div(flip, bit), 2) for bit in (1, 2, 4, 8))

    def to(place):
        return dict(device_id={"sp": place}, device_id_type=pl.DeviceIdType.MESH)

    def owner(j):
        return other(n - 1 - lax.div(lax.rem(j, turns), halves))

    def rows_of(j):
        return owner(j) * rounds + lax.div(j, turns), pl.multiple_of(lax.rem(j, halves) * STEP, STEP)

    def group(start, g):
        return pl.ds(pl.multiple_of(start + g * GROUP, GROUP), GROUP)

    def fetch_k(j):
        b, start = rows_of(j)
        slot = lax.rem(j, SLOTS)
        return pltpu.make_async_copy(k_ref.at[b, pl.ds(start, STEP)], keys.at[slot], k_sem.at[slot])

    def value_copy(j, g):
        b, start = rows_of(j)
        slot = lax.rem(j, SLOTS)
        return pltpu.make_async_copy(v_ref.at[b, group(start, g)], values.at[slot, group(0, g)], v_sem.at[slot, g])

    def fetch_v(j):
        @pl.loop(0, groups)
        def _(g):
            value_copy(j, g).start()

    def wait(ref, sem):
        pltpu.make_async_copy(ref, ref, sem).wait()

    query = pltpu.make_async_copy(q_hbm, q_ref, q_sem)
    query.start()

    @pl.loop(0, AHEAD)
    def _(j):
        fetch_k(j).start()

    @pl.loop(AHEAD, SLOTS)
    def _(j):
        fetch_k(j).start()
        fetch_v(j - AHEAD)

    @pl.loop(SLOTS - AHEAD, SLOTS)
    def _(j):
        fetch_v(j)

    barrier = pltpu.get_barrier_semaphore()

    @pl.loop(1, n)
    def _(flip):
        pl.semaphore_signal(barrier, inc=1, **to(other(flip)))

    pl.semaphore_wait(barrier, n - 1)
    query.wait()

    def weigh(j):
        b, start = rows_of(j)
        slot, turn = lax.rem(j, SLOTS), lax.rem(j, AHEAD + 1)
        for g in range(groups):
            weights, high, total = weights_of(q_ref[b, group(start, g)], lambda h: keys[slot, g * GROUP + h])
            kept[turn, group(0, g)] = weights
            kept_high[turn, group(0, g)] = jnp.broadcast_to(high, (GROUP, ROW))
            kept_total[turn, group(0, g)] = jnp.broadcast_to(total, (GROUP, ROW))

    def seen_of(j, g):
        slot, turn = lax.rem(j, SLOTS), lax.rem(j, AHEAD + 1)
        return over_heads(kept[turn, group(0, g)], lambda h: values[slot, g * GROUP + h], (1, 1))

    def next_fetch(j):
        @pl.when(j + AHEAD + SLOTS < steps)
        def _():
            fetch_k(j + AHEAD + SLOTS).start()

        @pl.when(j + SLOTS < steps)
        def _():
            fetch_v(j + SLOTS)

    def send_out(rows, flip):
        pltpu.make_async_remote_copy(rows, rows, send_sem, out_sem, **to(other(flip))).start()

    hops = {flip: (flip // 2).bit_count() for flip in range(1, n)}
    far = [flip for flip in sorted(hops, key=lambda flip: (-hops[flip], -(flip // 2), flip % 2)) if hops[flip] > 1]
    close = [flip for flip in range(n - 1, 0, -1) if hops[flip] < 2]

    @pl.loop(0, AHEAD)
    def _(j):
        fetch_k(j).wait()
        weigh(j)
        fetch_k(j + SLOTS).start()

    @pl.loop(0, rounds)
    def _(r):
        @pl.loop(0, turns - halves)
        def _(i):
            j, sent = r * turns + i, r * (turns - halves) + i
            place, half = owner(j), lax.rem(i, halves)
            turn, to_send = lax.rem(j, AHEAD + 1), lax.rem(sent, SENDS)
            fetch_k(j + AHEAD).wait()
            for g in range(groups):
                value_copy(j, g).wait()

            @pl.when(sent >= SENDS)
            def _():
                wait(part.at[to_send], part_sem.at[to_send])

            weigh(j + AHEAD)
            for g in range(groups):
                at = group(0, g)
                part[to_send, at, :HIGH] = seen_of(j, g)
                part[to_send, at, HIGH:TOTAL] = kept_high[turn, at, HIGH:TOTAL]
                part[to_send, at, TOTAL:] = kept_total[turn, at, TOTAL:]
            near = lax.div(i, halves * (n - 2))
            pltpu.make_async_remote_copy(part.at[to_send], got.at[r, half, me], part_sem.at[to_send], got_sem.at[r, half, near], **to(place)).start()
            next_fetch(j)

        for half in range(halves):
            j = (r + 1) * turns - halves + half
            b, start = rows_of(j)
            turn, last = lax.rem(j, AHEAD + 1), half == halves - 1
            seen = []
            if last:
                for g in range(groups - 1):
                    value_copy(j, g).wait()
                    seen.append(seen_of(j, g))
            for g in range(len(seen), groups):
                value_copy(j, g).wait()
            wait(got.at[r, half, pl.ds(0, n - 2)], got_sem.at[r, half, 0])
            wait(got.at[r, half, other(1)], got_sem.at[r, half, 1])
            seen += [seen_of(j, g) for g in range(len(seen), groups)]
            for g in range(groups):
                parts = [got[r, half, other(flip), group(0, g)] for flip in range(1, n)]
                high = kept_high[turn, group(0, g), :1]
                top = functools.reduce(jnp.maximum, [x[:, HIGH:HIGH + 1] for x in parts], high)
                new = jnp.exp(high - top)
                rest = sum(x * jnp.exp(x[:, HIGH:HIGH + 1] - top) for x in parts)
                total = rest[:, TOTAL:TOTAL + 1] + kept_total[turn, group(0, g), :1] * new
                at = out_ref.at[b, group(start, g)]
                at[...] = (rest[:, :HIGH] / total + seen[g] * (new / total)).astype(out_ref.dtype)
            for flip in far:
                send_out(out_ref.at[b, pl.ds(start, STEP)], flip)
            if last:
                for flip in close:
                    send_out(out_ref.at[b], flip)

            @pl.when(j + AHEAD < steps)
            def _():
                fetch_k(j + AHEAD).wait()
                weigh(j + AHEAD)

            next_fetch(j)

    for turn in range(SENDS):
        wait(part.at[turn], part_sem.at[turn])
    wait(out_ref.at[pl.ds(0, batch - rounds)], send_sem)
    wait(out_ref.at[pl.ds(0, batch - rounds)], out_sem)


def solution(mesh):
    n = mesh.shape["sp"]

    def step(q, k, v):
        batch, keys, heads, head = k.shape
        rounds, halves, groups = batch // n, heads // STEP, STEP // GROUP
        return pl.pallas_call(
            functools.partial(kernel, n),
            out_shape=jax.ShapeDtypeStruct(q.shape, q.dtype),
            in_specs=[pl.BlockSpec(memory_space=pl.ANY)] * 3,
            out_specs=pl.BlockSpec(memory_space=pltpu.VMEM),
            scratch_shapes=[
                pltpu.VMEM(q.shape, q.dtype),
                pltpu.VMEM((SLOTS, STEP, head, keys), k.dtype),
                pltpu.VMEM((SLOTS, STEP, head, keys), v.dtype),
                pltpu.VMEM((SENDS, STEP, ROW), jnp.float32),
                pltpu.VMEM((rounds, halves, n, STEP, ROW), jnp.float32),
                pltpu.VMEM((AHEAD + 1, STEP, keys), q.dtype),
                pltpu.VMEM((AHEAD + 1, STEP, ROW), jnp.float32),
                pltpu.VMEM((AHEAD + 1, STEP, ROW), jnp.float32),
                pltpu.SemaphoreType.DMA,
                pltpu.SemaphoreType.DMA((SLOTS,)),
                pltpu.SemaphoreType.DMA((SLOTS, groups)),
                pltpu.SemaphoreType.DMA((SENDS,)),
                pltpu.SemaphoreType.DMA((rounds, halves, 2)),
                pltpu.SemaphoreType.DMA,
                pltpu.SemaphoreType.DMA,
            ],
            compiler_params=pltpu.CompilerParams(collective_id=0, has_side_effects=True, vmem_limit_bytes=48 * 2**20),
        )(pltpu.with_memory_space_constraint(q, pltpu.HBM), jnp.transpose(k, (0, 2, 3, 1)), jnp.transpose(v, (0, 2, 3, 1)))

    return jax.shard_map(
        step,
        mesh=mesh,
        in_specs=(P("dp", None, None), P("dp", "sp", None, None), P("dp", "sp", None, None)),
        out_specs=P("dp", None, None),
        check_vma=False,
    )
```
